32 devices in a mesh: seq: 8 (over z, x), head: 4 (over y, core).
Axes of the slice: x: 2, y: 2, z: 4, core: 2. Of those that a mesh axis runs over, the one named last changes fastest.
Arguments:
- features: bfloat16 [2048, 1024], P('seq', 'head'), may hold values from -6 to 6
- w_query: bfloat16 [1024, 512], P(None, 'head'), may hold values from -0.1875 to 0.1875
- w_key: bfloat16 [1024, 512], P(None, 'head'), may hold values from -0.1875 to 0.1875
- w_value: bfloat16 [1024, 1024], P(None, 'head'), may hold values from -0.1875 to 0.1875
- w_gate: bfloat16 [1024, 1024], P(None, 'head'), may hold values from -0.1875 to 0.1875
- w_out: bfloat16 [1024, 1024], replicated, may hold values from -0.1875 to 0.1875
- forget: bfloat16 [2, 2048, 512], P(None, 'seq', 'head'), may hold values from -2.5 to 0, as said below
Outputs:
- encoded: bfloat16 [2048, 1024], P('seq', 'head')
The draws below stay inside these ranges and needn't reach their ends.
Inputs may be any that keep to these rules, and one draw needn't show every extreme that they name: `forget`: every entry is below zero.
All inputs are finite; a program needn't handle non-finite values.
Results may differ from the reference program's by a relative error of at most 0.013.
Values may be sent and summed in bfloat16 or wider, within the bound.
A program may use at most 64 MiB of HBM per device.

```python
import math
import jax
import jax.numpy as jnp
from jax import lax

D = 1024
HEADS = 8
HEAD_K = 64
HEAD_V = 128
GROUP = 64
TOK_DEV = 256
TOKENS = 2048
KEY_W = 512
VAL_W = 1024


def draw_forget(key, part):
    subkeys = jax.random.split(key, 7)
    slow_share = 0.5
    block_total = TOKENS // TOK_DEV
    slow_mask = jax.random.uniform(subkeys[0], (2, 1, 1, KEY_W)) < slow_share
    slow_rate = jnp.exp(jax.random.uniform(subkeys[1], (2, 1, 1, KEY_W), minval=math.log(0.1), maxval=0.0)) / TOKENS
    fast_rate = jnp.exp(jax.random.uniform(subkeys[2], (2, 1, 1, KEY_W), minval=math.log(1.0 / 400.0), maxval=math.log(1.0 / 30.0)))
    base_rate = jnp.where(slow_mask, slow_rate, fast_rate)
    device_factor = jnp.exp(jax.random.uniform(subkeys[3], (2, block_total, 1, KEY_W), minval=-math.log(2.0), maxval=math.log(2.0)))
    roughness = jax.random.uniform(subkeys[4], (2, block_total, TOK_DEV, KEY_W), minval=0.5, maxval=1.5)
    stable_level = (base_rate * device_factor * roughness).reshape(2, TOKENS, KEY_W)
    spots = jax.random.randint(subkeys[5], (2, 1, 3), 0, TOKENS)
    layer_depth_values = jax.random.uniform(subkeys[6], (2, 1, 3), minval=math.log(1.25), maxval=math.log(2.0))
    match_positions = (jnp.arange(TOKENS)[None, :, None] == spots).astype(jnp.float32)
    sudden_spikes = jnp.sum(match_positions * layer_depth_values, axis=2)[:, :, None]
    return (-(stable_level + sudden_spikes)).astype(jnp.bfloat16)


def block_scale(stream_key, shape, cuts, least, high):
    def one(position, parts):
        draws = jax.random.uniform(jax.random.fold_in(jax.random.fold_in(stream_key, 6), position), (parts,), jnp.float32, least / len(cuts), high / len(cuts))
        return jnp.repeat(jnp.exp(draws), shape[position] // parts).reshape((-1,) + (1,) * (len(shape) - position - 1))

    level = one(*cuts[0])
    for cut in cuts[1:]:
        level = level * one(*cut)
    return level


def normal_values(rng, dims, deviation, limit, cuts=(), kind=jnp.bfloat16):
    array = deviation * jax.random.normal(rng, dims, jnp.float32)
    if cuts:
        array = array * block_scale(rng, dims, cuts, -0.22, 0.18)
    return jnp.clip(array, -limit, limit).astype(kind)


def setup_inputs(seed: int = 0) -> dict:
    key_list = jax.random.split(jax.random.key(seed), 8)
    features = normal_values(key_list[0], (TOKENS, D), 1.0, 6.0, ((0, 8), (1, 4)))
    w_query = normal_values(key_list[1], (D, KEY_W), D ** -0.5, 0.1875, ((1, 4),))
    w_key = normal_values(key_list[2], (D, KEY_W), D ** -0.5, 0.1875, ((1, 4),))
    w_value = normal_values(key_list[3], (D, VAL_W), D ** -0.5, 0.1875, ((1, 4),))
    w_gate = normal_values(key_list[4], (D, VAL_W), D ** -0.5, 0.1875, ((1, 4),))
    w_out = normal_values(key_list[5], (VAL_W, D), VAL_W ** -0.5, 0.1875)
    forget = draw_forget(jax.random.fold_in(key_list[7], 71), 0)
    return {"features": features, "w_query": w_query, "w_key": w_key, "w_value": w_value, "w_gate": w_gate, "w_out": w_out, "forget": forget}


def block_pass(query_matrix, key_rows, value_rows, decays, initial):
    block_count = query_matrix.shape[0] // GROUP
    triangle = jnp.tril(jnp.ones((GROUP, GROUP), jnp.float32))

    def advance(memory, blocks):
        query_block, key_block, value_block, decay_block = blocks
        running = jnp.cumsum(decay_block, axis=0)
        query_decayed = (query_block.astype(jnp.float32) * jnp.exp(running)).astype(jnp.bfloat16).astype(jnp.float32)
        key_grown = (key_block.astype(jnp.float32) * jnp.exp(-running)).astype(jnp.bfloat16).astype(jnp.float32)
        value_float = value_block.astype(jnp.float32)
        scores = jnp.einsum('thi,shi->hts', query_decayed, key_grown, precision=lax.Precision.HIGHEST) * triangle
        scores = scores.astype(jnp.bfloat16).astype(jnp.float32)
        within = jnp.einsum('hts,shj->thj', scores, value_float, precision=lax.Precision.HIGHEST)
        carried = jnp.einsum('thi,hij->thj', query_decayed, memory, precision=lax.Precision.HIGHEST)
        finale = running[-1]
        key_to_end = (key_block.astype(jnp.float32) * jnp.exp(finale[None] - running)).astype(jnp.bfloat16).astype(jnp.float32)
        memory = jnp.exp(finale)[:, :, None] * memory + jnp.einsum('shi,shj->hij', key_to_end, value_float, precision=lax.Precision.HIGHEST)
        return (memory, within + carried)
    blocks = tuple((tensor.reshape((block_count, GROUP) + tensor.shape[1:]) for tensor in (query_matrix, key_rows, value_rows, decays)))
    last_memory, outputs = lax.scan(advance, initial, blocks)
    return outputs.reshape((block_count * GROUP,) + outputs.shape[2:])

def reference(features, w_query, w_key, w_value, w_gate, w_out, forget):
    query_matrix = (jnp.dot(features, w_query, preferred_element_type=jnp.float32) * 0.125).astype(jnp.bfloat16).reshape(TOKENS, HEADS, HEAD_K)
    key_rows = jnp.dot(features, w_key, preferred_element_type=jnp.float32).astype(jnp.bfloat16).reshape(TOKENS, HEADS, HEAD_K)
    value_rows = jnp.dot(features, w_value, preferred_element_type=jnp.float32).astype(jnp.bfloat16).reshape(TOKENS, HEADS, HEAD_V)
    gating = jnp.dot(features, w_gate, preferred_element_type=jnp.float32)
    decays = forget.astype(jnp.float32).reshape(2, TOKENS, HEADS, HEAD_K)
    blank_memory = jnp.zeros((HEADS, HEAD_K, HEAD_V), jnp.float32)
    ahead_out = block_pass(query_matrix, key_rows, value_rows, decays[0], blank_memory)
    behind_out = jnp.flip(block_pass(jnp.flip(query_matrix, 0), jnp.flip(key_rows, 0), jnp.flip(value_rows, 0), jnp.flip(decays[1], 0), blank_memory), 0)
    mixture = ahead_out + behind_out
    scaled = mixture * lax.rsqrt(lax.optimization_barrier(jnp.mean(mixture * mixture, axis=-1, keepdims=True)) + 1e-06)
    normed = (scaled.reshape(TOKENS, VAL_W) * jax.nn.silu(gating)).astype(jnp.bfloat16)
    return jnp.dot(normed, w_out, preferred_element_type=jnp.float32).astype(jnp.bfloat16)
```

```python
import functools

import jax
import jax.numpy as jnp
from jax import lax
from jax.experimental import pallas as pl
from jax.experimental.pallas import tpu as pltpu
from jax.sharding import PartitionSpec as P

HEAD_K = 64
HEAD_V = 128
GROUP = 64
CHUNKS = 2
MESH = pl.DeviceIdType.MESH
F32 = jnp.float32
BF16 = jnp.bfloat16
NT = (((1,), (1,)), ((), ()))
TN = (((0,), (0,)), ((), ()))


def dot(a, b):
    return jnp.dot(a, b, preferred_element_type=F32)


def each(count, start, body):
    if count - start <= 16:
        for i in range(start, count):
            body(i)
    else:
        lax.fori_loop(start, count, lambda i, c: (body(i), c)[1], 0)


class HeadGather:
    def __init__(self, heads, me, own, slots, rows, cs, cr, ss, sr):
        self.chips = heads // 2
        self.core = lax.rem(me, 2)
        self.chip = lax.div(me, 2)
        self.me, self.own, self.slots, self.rows = me, own, slots, rows
        self.sib = me + 1 - 2 * self.core
        self.cs, self.cr, self.ss, self.sr = cs, cr, ss, sr
        self.started = []

    def cut(self, ref, c):
        return ref.at[pl.ds(c * self.rows, self.rows), :]

    def cross_origin(self, j):
        return lax.rem(self.chip - j + self.chips, self.chips) * 2 + self.core

    def handed_origin(self, j):
        return lax.rem(self.chip - j + self.chips, self.chips) * 2 + 1 - self.core

    def cross(self, j, c):
        target = lax.rem(self.chip + j, self.chips) * 2 + self.core
        return pltpu.make_async_remote_copy(
            src_ref=self.cut(self.own, c),
            dst_ref=self.cut(self.slots.at[self.me], c),
            send_sem=self.cs.at[j, c],
            recv_sem=self.cr.at[j, c],
            device_id={"head": target},
            device_id_type=MESH,
        )

    def side(self, j, c):
        origin = self.me if j == 0 else self.cross_origin(j)
        src = self.own if j == 0 else self.slots.at[origin]
        return pltpu.make_async_remote_copy(
            src_ref=self.cut(src, c),
            dst_ref=self.cut(self.slots.at[origin], c),
            send_sem=self.ss.at[j, c],
            recv_sem=self.sr.at[j, c],
            device_id={"head": self.sib},
            device_id_type=MESH,
        )

    def start(self, c):
        for j in range(1, self.chips):
            copy = self.cross(j, c)
            copy.start()
            self.started.append(copy)
        copy = self.side(0, c)
        copy.start()
        self.started.append(copy)

    def hand_on(self, j, c):
        self.cross(j, c).wait_recv()
        copy = self.side(j, c)
        copy.start()
        self.started.append(copy)

    def finish(self):
        for copy in self.started:
            copy.wait_send()


def kernel(
    heads, seqs,
    feat_hbm, wq_hbm, wk_hbm, wv_hbm, wg_hbm, wo_hbm, forget_hbm,
    out_ref,
    feat, w_s, wo_s, fg, acc, mults, edge, tots, wts, st, recv, vals, keys, ps, mix, nrm,
    own_sem, w_sem, wo_sem, fg_sem,
    fcs, fcr, fss, fsr, ncs, ncr, nss, nsr, ts, tr, xs, xr,
):
    h = lax.axis_index("head")
    p = lax.axis_index("seq")
    rows, width = feat_hbm.shape
    kw = wq_hbm.shape[1]
    vw = wv_hbm.shape[1]
    blocks = rows // GROUP
    crows = rows // CHUNKS
    k0, v0, q0, g0 = 0, kw, kw + vw, kw + vw + kw

    fg_copy = pltpu.make_async_copy(forget_hbm, fg, fg_sem)
    fg_copy.start()
    own_copy = pltpu.make_async_copy(feat_hbm, feat.at[h], own_sem)
    own_copy.start()
    w_copies = []
    for i in range(heads):
        for n, (src, at, wide) in enumerate(
            ((wk_hbm, k0, kw), (wv_hbm, v0, vw), (wq_hbm, q0, kw), (wg_hbm, g0, vw))
        ):
            copy = pltpu.make_async_copy(
                src.at[pl.ds(i * width, width), :],
                w_s.at[i, :, pl.ds(at, wide)],
                w_sem.at[i, n],
            )
            copy.start()
            w_copies.append(copy)
    wo_copies = []
    ow = out_ref.shape[1]
    for i in range(heads):
        copy = pltpu.make_async_copy(
            wo_hbm.at[pl.ds(i * vw, vw), pl.ds(pl.multiple_of(h * ow, ow), ow)],
            wo_s.at[i],
            wo_sem.at[i],
        )
        copy.start()
        wo_copies.append(copy)

    barrier = pltpu.get_barrier_semaphore()
    for j in range(1, heads):
        pl.semaphore_signal(
            barrier, inc=1, device_id={"head": lax.rem(h + j, heads)}, device_id_type=MESH
        )
    each(
        seqs,
        1,
        lambda d: pl.semaphore_signal(
            barrier, inc=1, device_id={"seq": lax.rem(p + d, seqs)}, device_id_type=MESH
        ),
    )
    pl.semaphore_wait(barrier, heads - 1 + seqs - 1)

    gather = HeadGather(heads, h, feat_hbm, feat, crows, fcs, fcr, fss, fsr)
    for c in range(CHUNKS):
        gather.start(c)

    fg_copy.wait()
    tok = lax.broadcasted_iota(jnp.int32, (rows, rows), 0)
    src = lax.broadcasted_iota(jnp.int32, (rows, rows), 1)
    same = (tok // GROUP) == (src // GROUP)
    row = lax.broadcasted_iota(jnp.int32, (rows, kw), 0)
    lane = lax.broadcasted_iota(jnp.int32, (rows, kw), 1)
    edge[...] = jnp.zeros_like(edge)
    whole_sums, block_sums = [], []
    for d in range(2):
        order = (src <= tok) if d == 0 else (src >= tok)
        f = fg[d]
        whole = dot(jnp.where(order, 1.0, 0.0).astype(BF16), f)
        block = dot(jnp.where(order & same, 1.0, 0.0).astype(BF16), f)
        total = whole[rows - 1 : rows] if d == 0 else whole[0:1]
        edge[d : d + 1, :] = total
        whole_sums.append(whole)
        block_sums.append(block)

    def total_copy(d):
        return pltpu.make_async_remote_copy(
            src_ref=edge,
            dst_ref=tots.at[p],
            send_sem=ts.at[d],
            recv_sem=tr.at[d],
            device_id={"seq": lax.rem(p + d, seqs)},
            device_id_type=MESH,
        )

    for d in range(2):
        whole, block = whole_sums[d], block_sums[d]
        total = whole[rows - 1 : rows] if d == 0 else whole[0:1]
        mults[d, blocks] = jnp.exp(block)
        mults[d, blocks + 1] = jnp.exp(total - whole)
        mults[d, blocks + 2] = jnp.exp(whole)
        for i in range(blocks):
            lo, hi = i * GROUP, (i + 1) * GROUP
            inside = (row >= lo) & (row < hi)
            if d == 0:
                past = row < lo
                start = whole[lo - 1 : lo] if i else jnp.zeros((1, kw), F32)
            else:
                past = row >= hi
                start = whole[hi : hi + 1] if i < blocks - 1 else jnp.zeros((1, kw), F32)
            power = jnp.where(past, start - whole, jnp.where(inside, -block, -jnp.inf))
            mults[d, i] = jnp.exp(power)
    each(seqs, 1, lambda d: total_copy(d).start())

    own_copy.wait()
    for copy in w_copies:
        copy.wait()
    acc[...] = dot(feat[h], w_s[h])
    gather.hand_on(1, 0)
    for c in range(CHUNKS):
        gather.side(0, c).wait_recv()
    acc[...] += dot(feat[gather.sib], w_s[gather.sib])
    for j in range(1, gather.chips):
        for c in range(CHUNKS):
            if j > 1 or c > 0:
                gather.hand_on(j, c)
        at = gather.cross_origin(j)
        if j < gather.chips - 1:
            acc[...] += dot(feat[at], w_s[at])
        else:
            acc[...] += dot(feat[at], w_s[at])
        for c in range(CHUNKS):
            gather.side(j, c).wait_recv()
        at = gather.handed_origin(j)
        if j < gather.chips - 1:
            acc[...] += dot(feat[at], w_s[at])
    last = gather.handed_origin(gather.chips - 1)
    kv = acc[:, :q0] + dot(feat[last], w_s[last, :, :q0])
    key = kv[:, :kw].astype(BF16)
    val = kv[:, kw:].astype(BF16)
    keys[...] = key
    vals[...] = val

    keyf = key.astype(F32)
    grown = jnp.concatenate(
        [(keyf * mults[d, blocks + 1]).astype(BF16) for d in range(2)], axis=1
    )
    state = lax.dot_general(val, grown, TN, preferred_element_type=F32)
    slane = lax.broadcasted_iota(jnp.int32, (HEAD_V, kw), 1)
    heads_here = kw // HEAD_K
    for d in range(2):
        packed = state[:HEAD_V, d * kw : (d + 1) * kw]
        for g in range(1, heads_here):
            packed = jnp.where(
                slane >= g * HEAD_K,
                state[g * HEAD_V : (g + 1) * HEAD_V, d * kw : (d + 1) * kw],
                packed,
            )
        st[d] = packed.astype(BF16)

    def state_copy(d):
        q = lax.rem(p + d, seqs)
        return pltpu.make_async_remote_copy(
            src_ref=st.at[jnp.where(q > p, 0, 1)],
            dst_ref=recv.at[p],
            send_sem=xs.at[d],
            recv_sem=xr.at[d],
            device_id={"seq": q},
            device_id_type=MESH,
        )

    each(seqs, 1, lambda d: state_copy(d).start())

    qg = acc[:, q0:] + dot(feat[last], w_s[last, :, q0:])
    query = (qg[:, :kw] * 0.125).astype(BF16).astype(F32)
    gate = qg[:, kw:]
    acc[:, :vw] = gate / (1.0 + jnp.exp(-gate))
    qd = [(query * mults[d, blocks]).astype(BF16) for d in range(2)]
    qdev = jnp.concatenate(
        [(query * mults[d, blocks + 2]).astype(BF16) for d in range(2)], axis=1
    )
    blane = lax.broadcasted_iota(jnp.int32, (GROUP, kw), 1) // HEAD_K
    bt = lax.rem(lax.broadcasted_iota(jnp.int32, (heads_here * GROUP, rows), 0), GROUP)
    bs = lax.broadcasted_iota(jnp.int32, (heads_here * GROUP, rows), 1)
    for i in range(blocks):
        scores = []
        for d in range(2):
            qb = qd[d][i * GROUP : (i + 1) * GROUP]
            stacked = jnp.concatenate(
                [jnp.where(blane == g, qb, jnp.zeros_like(qb)) for g in range(heads_here)], axis=0
            )
            grown_keys = (keyf * mults[d, i]).astype(BF16)
            part = lax.dot_general(stacked, grown_keys, NT, preferred_element_type=F32)
            keep = (bs <= bt + i * GROUP) if d == 0 else (bs >= bt + i * GROUP)
            scores.append(jnp.where(keep, part, 0.0))
        both = (scores[0] + scores[1]).astype(BF16)
        for g in range(heads_here):
            ps[g, i * GROUP : (i + 1) * GROUP, :] = both[g * GROUP : (g + 1) * GROUP]
    for g in range(heads_here):
        cols = slice(g * HEAD_V, (g + 1) * HEAD_V)
        mix[:, cols] = dot(ps[g], val[:, cols])

    each(seqs, 1, lambda d: total_copy(d).wait_recv())
    tots[p] = jnp.zeros_like(edge)

    def weigh(j, sums):
        ahead, behind = sums
        k = p - j
        ok = k >= 0
        at = jnp.maximum(k, 0)
        wts[j, 0:1, :] = jnp.where(ok, jnp.exp(ahead), 0.0)
        ahead = ahead + jnp.where(ok, tots[at, 0:1, :], 0.0)
        k = p + j
        ok = k < seqs
        at = jnp.minimum(k, seqs - 1)
        wts[seqs - j, 1:2, :] = jnp.where(ok, jnp.exp(behind), 0.0)
        behind = behind + jnp.where(ok, tots[at, 1:2, :], 0.0)
        return ahead, behind

    zero = jnp.zeros((1, kw), F32)
    sums = (zero, zero)
    if seqs <= 16:
        for j in range(1, seqs):
            sums = weigh(j, sums)
    else:
        lax.fori_loop(1, seqs, weigh, sums)

    def gain(d, inflow):
        state_copy(d).wait_recv()
        part = recv[lax.rem(p - d + seqs, seqs)].astype(F32)
        return inflow[0] + part * wts[d, 0:1, :], inflow[1] + part * wts[d, 1:2, :]

    none = jnp.zeros((HEAD_V, kw), F32)
    inflow = (none, none)
    if seqs <= 16:
        for d in range(1, seqs):
            inflow = gain(d, inflow)
    else:
        inflow = lax.fori_loop(1, seqs, gain, inflow)
    spread = jnp.concatenate(
        [
            jnp.concatenate(
                [jnp.where(slane // HEAD_K == g, inflow[d], 0.0) for g in range(heads_here)], axis=0
            )
            for d in range(2)
        ],
        axis=1,
    ).astype(BF16)

    tail = HeadGather(heads, h, nrm.at[h], nrm, crows, ncs, ncr, nss, nsr)
    for c in range(CHUNKS):
        at = slice(c * crows, (c + 1) * crows)
        whole = mix[at, :] + lax.dot_general(qdev[at], spread, NT, preferred_element_type=F32)
        for g in range(heads_here):
            cols = slice(g * HEAD_V, (g + 1) * HEAD_V)
            part = whole[:, cols]
            scale = lax.rsqrt(jnp.mean(part * part, axis=-1, keepdims=True) + 1e-06)
            nrm[h, at, cols] = (part * scale * acc[at, cols]).astype(BF16)
        tail.start(c)

    for copy in wo_copies:
        copy.wait()
    for c in range(CHUNKS):
        at = slice(c * crows, (c + 1) * crows)
        total = dot(nrm[h, at, :], wo_s[h])
        tail.side(0, c).wait_recv()
        total += dot(nrm[tail.sib, at, :], wo_s[tail.sib])
        for j in range(1, tail.chips):
            tail.hand_on(j, c)
            origin = tail.cross_origin(j)
            total += dot(nrm[origin, at, :], wo_s[origin])
            tail.side(j, c).wait_recv()
            origin = tail.handed_origin(j)
            total += dot(nrm[origin, at, :], wo_s[origin])
        out_ref[at, :] = total.astype(BF16)

    gather.finish()
    tail.finish()
    each(seqs, 1, lambda d: total_copy(d).wait_send())
    each(seqs, 1, lambda d: state_copy(d).wait_send())


def solution(mesh):
    heads, seqs = mesh.shape["head"], mesh.shape["seq"]

    def local(features, w_query, w_key, w_value, w_gate, w_out, forget):
        rows, width = features.shape
        kw, vw = w_query.shape[1], w_value.shape[1]
        ow = w_out.shape[1] // heads
        blocks = rows // GROUP
        chips = heads // 2
        dma = pltpu.SemaphoreType.DMA
        hop = dma((chips, CHUNKS))
        return pl.pallas_call(
            functools.partial(kernel, heads, seqs),
            out_shape=jax.ShapeDtypeStruct((rows, ow), BF16),
            in_specs=[pl.BlockSpec(memory_space=pl.ANY)] * 7,
            out_specs=pl.BlockSpec(memory_space=pltpu.VMEM),
            scratch_shapes=[
                pltpu.VMEM((heads, rows, width), BF16),
                pltpu.VMEM((heads, width, 2 * (kw + vw)), BF16),
                pltpu.VMEM((heads, vw, ow), BF16),
                pltpu.VMEM((2, rows, kw), BF16),
                pltpu.VMEM((rows, 2 * (kw + vw)), F32),
                pltpu.VMEM((2, blocks + 3, rows, kw), F32),
                pltpu.VMEM((8, kw), F32),
                pltpu.VMEM((seqs, 8, kw), F32),
                pltpu.VMEM((seqs, 8, kw), F32),
                pltpu.VMEM((2, HEAD_V, kw), BF16),
                pltpu.VMEM((seqs, HEAD_V, kw), BF16),
                pltpu.VMEM((rows, vw), BF16),
                pltpu.VMEM((rows, kw), BF16),
                pltpu.VMEM((kw // HEAD_K, rows, rows), BF16),
                pltpu.VMEM((rows, vw), F32),
                pltpu.VMEM((heads, rows, vw), BF16),
                dma,
                dma((heads, 4)),
                dma((heads,)),
                dma,
                hop, hop, hop, hop, hop, hop, hop, hop,
                dma((seqs,)), dma((seqs,)), dma((seqs,)), dma((seqs,)),
            ],
            compiler_params=pltpu.CompilerParams(
                collective_id=0, has_side_effects=True, vmem_limit_bytes=40 * 1024 * 1024
            ),
        )(features, w_query, w_key, w_value, w_gate, w_out, forget)

    placed = (
        P("seq", "head"),
        P(None, "head"),
        P(None, "head"),
        P(None, "head"),
        P(None, "head"),
        P(),
        P(None, "seq", "head"),
    )
    return jax.shard_map(
        local, mesh=mesh, in_specs=placed, out_specs=P("seq", "head"), check_vma=False
    )
```

```python
import functools

import jax
import jax.numpy as jnp
from jax import lax
from jax.experimental import pallas as pl
from jax.experimental.pallas import tpu as pltpu
from jax.sharding import PartitionSpec as P

HEAD_K = 64
HEAD_V = 128
GROUP = 64
CHUNKS = 2
MESH = pl.DeviceIdType.MESH
F32 = jnp.float32
BF16 = jnp.bfloat16
NT = (((1,), (1,)), ((), ()))
TN = (((0,), (0,)), ((), ()))


def dot(a, b):
    return jnp.dot(a, b, preferred_element_type=F32)


def each(count, start, body):
    if count - start <= 16:
        for i in range(start, count):
            body(i)
    else:
        lax.fori_loop(start, count, lambda i, c: (body(i), c)[1], 0)


class HeadGather:
    def __init__(self, heads, me, own, slots, rows, cs, cr, ss, sr):
        self.chips = heads // 2
        self.core = lax.rem(me, 2)
        self.chip = lax.div(me, 2)
        self.me, self.own, self.slots, self.rows = me, own, slots, rows
        self.sib = me + 1 - 2 * self.core
        self.cs, self.cr, self.ss, self.sr = cs, cr, ss, sr
        self.started = []

    def cut(self, ref, c):
        return ref.at[pl.ds(c * self.rows, self.rows), :]

    def cross_origin(self, j):
        return lax.rem(self.chip - j + self.chips, self.chips) * 2 + self.core

    def handed_origin(self, j):
        return lax.rem(self.chip - j + self.chips, self.chips) * 2 + 1 - self.core

    def cross(self, j, c):
        target = lax.rem(self.chip + j, self.chips) * 2 + self.core
        return pltpu.make_async_remote_copy(
            src_ref=self.cut(self.own, c),
            dst_ref=self.cut(self.slots.at[self.me], c),
            send_sem=self.cs.at[j, c],
            recv_sem=self.cr.at[j, c],
            device_id={"head": target},
            device_id_type=MESH,
        )

    def side(self, j, c):
        origin = self.me if j == 0 else self.cross_origin(j)
        src = self.own if j == 0 else self.slots.at[origin]
        return pltpu.make_async_remote_copy(
            src_ref=self.cut(src, c),
            dst_ref=self.cut(self.slots.at[origin], c),
            send_sem=self.ss.at[j, c],
            recv_sem=self.sr.at[j, c],
            device_id={"head": self.sib},
            device_id_type=MESH,
        )

    def start(self, c):
        for j in range(1, self.chips):
            copy = self.cross(j, c)
            copy.start()
            self.started.append(copy)
        copy = self.side(0, c)
        copy.start()
        self.started.append(copy)

    def hand_on(self, j, c):
        self.cross(j, c).wait_recv()
        copy = self.side(j, c)
        copy.start()
        self.started.append(copy)

    def finish(self):
        for copy in self.started:
            copy.wait_send()


def kernel(
    heads, seqs,
    feat_hbm, wq_hbm, wk_hbm, wv_hbm, wg_hbm, wo_hbm, forget_hbm,
    out_ref,
    feat, w_s, wo_s, fg, acc, mults, edge, tots, wts, st, recv, vals, keys, ps, mix, nrm,
    own_sem, w_sem, wo_sem, fg_sem,
    fcs, fcr, fss, fsr, ncs, ncr, nss, nsr, ts, tr, xs, xr, meet,
):
    h = lax.axis_index("head")
    p = lax.axis_index("seq")
    rows, width = feat_hbm.shape
    kw = wq_hbm.shape[1]
    vw = wv_hbm.shape[1]
    blocks = rows // GROUP
    crows = rows // CHUNKS
    k0, v0, q0, g0 = 0, kw, kw + vw, kw + vw + kw

    fg_copy = pltpu.make_async_copy(forget_hbm, fg, fg_sem)
    fg_copy.start()
    own_copy = pltpu.make_async_copy(feat_hbm, feat.at[h], own_sem)
    own_copy.start()
    w_copies = []
    for i in range(heads):
        for n, (src, at, wide) in enumerate(
            ((wk_hbm, k0, kw), (wv_hbm, v0, vw), (wq_hbm, q0, kw), (wg_hbm, g0, vw))
        ):
            copy = pltpu.make_async_copy(
                src.at[pl.ds(i * width, width), :],
                w_s.at[i, :, pl.ds(at, wide)],
                w_sem.at[i, n],
            )
            copy.start()
            w_copies.append(copy)
    wo_copies = []
    ow = out_ref.shape[1]
    for i in range(heads):
        copy = pltpu.make_async_copy(
            wo_hbm.at[pl.ds(i * vw, vw), pl.ds(pl.multiple_of(h * ow, ow), ow)],
            wo_s.at[i],
            wo_sem.at[i],
        )
        copy.start()
        wo_copies.append(copy)

    def near(sem, d):
        @pl.when(p >= d)
        def _():
            pl.semaphore_signal(sem, inc=1, device_id={"seq": p - d}, device_id_type=MESH)

        @pl.when(p + d < seqs)
        def _():
            pl.semaphore_signal(sem, inc=1, device_id={"seq": p + d}, device_id_type=MESH)

    def near_count(d):
        return jnp.where(p >= d, 1, 0) + jnp.where(p + d < seqs, 1, 0)

    barrier = pltpu.get_barrier_semaphore()
    sibling = h + 1 - 2 * lax.rem(h, 2)
    pl.semaphore_signal(barrier, inc=1, device_id={"head": sibling}, device_id_type=MESH)
    for j in range(2, heads, 2):
        pl.semaphore_signal(
            barrier, inc=1, device_id={"head": lax.rem(h + j, heads)}, device_id_type=MESH
        )
    near(barrier, 1)
    pl.semaphore_wait(barrier, heads // 2 + near_count(1))

    rounds = meet.shape[0]
    near(meet.at[0], 1)

    def met(r):
        pl.semaphore_wait(meet.at[r], near_count(1 << r))
        if r + 1 < rounds:
            near(meet.at[r + 1], 1 << (r + 1))

    gather = HeadGather(heads, h, feat_hbm, feat, crows, fcs, fcr, fss, fsr)
    for c in range(CHUNKS):
        gather.start(c)

    fg_copy.wait()
    tok = lax.broadcasted_iota(jnp.int32, (rows, rows), 0)
    src = lax.broadcasted_iota(jnp.int32, (rows, rows), 1)
    same = (tok // GROUP) == (src // GROUP)
    row = lax.broadcasted_iota(jnp.int32, (rows, kw), 0)
    lane = lax.broadcasted_iota(jnp.int32, (rows, kw), 1)
    edge[...] = jnp.zeros_like(edge)
    whole_sums, block_sums = [], []
    for d in range(2):
        order = (src <= tok) if d == 0 else (src >= tok)
        f = fg[d]
        whole = dot(jnp.where(order, 1.0, 0.0).astype(BF16), f)
        block = dot(jnp.where(order & same, 1.0, 0.0).astype(BF16), f)
        total = whole[rows - 1 : rows] if d == 0 else whole[0:1]
        edge[d : d + 1, :] = total
        whole_sums.append(whole)
        block_sums.append(block)

    met(0)

    def total_copy(d):
        return pltpu.make_async_remote_copy(
            src_ref=edge,
            dst_ref=tots.at[p],
            send_sem=ts.at[d],
            recv_sem=tr.at[d],
            device_id={"seq": lax.rem(p + d, seqs)},
            device_id_type=MESH,
        )

    for d in range(2):
        whole, block = whole_sums[d], block_sums[d]
        total = whole[rows - 1 : rows] if d == 0 else whole[0:1]
        mults[d, blocks] = jnp.exp(block)
        mults[d, blocks + 1] = jnp.exp(total - whole)
        mults[d, blocks + 2] = jnp.exp(whole)
        for i in range(blocks):
            lo, hi = i * GROUP, (i + 1) * GROUP
            inside = (row >= lo) & (row < hi)
            if d == 0:
                past = row < lo
                start = whole[lo - 1 : lo] if i else jnp.zeros((1, kw), F32)
            else:
                past = row >= hi
                start = whole[hi : hi + 1] if i < blocks - 1 else jnp.zeros((1, kw), F32)
            power = jnp.where(past, start - whole, jnp.where(inside, -block, -jnp.inf))
            mults[d, i] = jnp.exp(power)
    if rounds > 1:
        met(1)

    own_copy.wait()
    for copy in w_copies:
        copy.wait()
    acc[...] = dot(feat[h], w_s[h])
    gather.hand_on(1, 0)
    for r in range(2, rounds):
        met(r)
    each(seqs, 1, lambda d: total_copy(d).start())
    for c in range(CHUNKS):
        gather.side(0, c).wait_recv()
    acc[...] += dot(feat[gather.sib], w_s[gather.sib])
    for j in range(1, gather.chips):
        for c in range(CHUNKS):
            if j > 1 or c > 0:
                gather.hand_on(j, c)
        at = gather.cross_origin(j)
        if j < gather.chips - 1:
            acc[...] += dot(feat[at], w_s[at])
        else:
            acc[...] += dot(feat[at], w_s[at])
        for c in range(CHUNKS):
            gather.side(j, c).wait_recv()
        at = gather.handed_origin(j)
        if j < gather.chips - 1:
            acc[...] += dot(feat[at], w_s[at])
    last = gather.handed_origin(gather.chips - 1)
    kv = acc[:, :q0] + dot(feat[last], w_s[last, :, :q0])
    key = kv[:, :kw].astype(BF16)
    val = kv[:, kw:].astype(BF16)
    keys[...] = key
    vals[...] = val

    keyf = key.astype(F32)
    grown = jnp.concatenate(
        [(keyf * mults[d, blocks + 1]).astype(BF16) for d in range(2)], axis=1
    )
    state = lax.dot_general(val, grown, TN, preferred_element_type=F32)
    slane = lax.broadcasted_iota(jnp.int32, (HEAD_V, kw), 1)
    heads_here = kw // HEAD_K
    for d in range(2):
        packed = state[:HEAD_V, d * kw : (d + 1) * kw]
        for g in range(1, heads_here):
            packed = jnp.where(
                slane >= g * HEAD_K,
                state[g * HEAD_V : (g + 1) * HEAD_V, d * kw : (d + 1) * kw],
                packed,
            )
        st[d] = packed.astype(BF16)

    def state_copy(d):
        q = lax.rem(p + d, seqs)
        return pltpu.make_async_remote_copy(
            src_ref=st.at[jnp.where(q > p, 0, 1)],
            dst_ref=recv.at[p],
            send_sem=xs.at[d],
            recv_sem=xr.at[d],
            device_id={"seq": q},
            device_id_type=MESH,
        )

    each(seqs, 1, lambda d: state_copy(d).start())

    qg = acc[:, q0:] + dot(feat[last], w_s[last, :, q0:])
    query = (qg[:, :kw] * 0.125).astype(BF16).astype(F32)
    gate = qg[:, kw:]
    acc[:, :vw] = gate / (1.0 + jnp.exp(-gate))
    qd = [(query * mults[d, blocks]).astype(BF16) for d in range(2)]
    qdev = jnp.concatenate(
        [(query * mults[d, blocks + 2]).astype(BF16) for d in range(2)], axis=1
    )
    blane = lax.broadcasted_iota(jnp.int32, (GROUP, kw), 1) // HEAD_K
    bt = lax.rem(lax.broadcasted_iota(jnp.int32, (heads_here * GROUP, rows), 0), GROUP)
    bs = lax.broadcasted_iota(jnp.int32, (heads_here * GROUP, rows), 1)
    for i in range(blocks):
        scores = []
        for d in range(2):
            qb = qd[d][i * GROUP : (i + 1) * GROUP]
            stacked = jnp.concatenate(
                [jnp.where(blane == g, qb, jnp.zeros_like(qb)) for g in range(heads_here)], axis=0
            )
            grown_keys = (keyf * mults[d, i]).astype(BF16)
            part = lax.dot_general(stacked, grown_keys, NT, preferred_element_type=F32)
            keep = (bs <= bt + i * GROUP) if d == 0 else (bs >= bt + i * GROUP)
            scores.append(jnp.where(keep, part, 0.0))
        both = (scores[0] + scores[1]).astype(BF16)
        for g in range(heads_here):
            ps[g, i * GROUP : (i + 1) * GROUP, :] = both[g * GROUP : (g + 1) * GROUP]
    for g in range(heads_here):
        cols = slice(g * HEAD_V, (g + 1) * HEAD_V)
        mix[:, cols] = dot(ps[g], val[:, cols])

    each(seqs, 1, lambda d: total_copy(d).wait_recv())
    tots[p] = jnp.zeros_like(edge)

    def weigh(j, sums):
        ahead, behind = sums
        k = p - j
        ok = k >= 0
        at = jnp.maximum(k, 0)
        wts[j, 0:1, :] = jnp.where(ok, jnp.exp(ahead), 0.0)
        ahead = ahead + jnp.where(ok, tots[at, 0:1, :], 0.0)
        k = p + j
        ok = k < seqs
        at = jnp.minimum(k, seqs - 1)
        wts[seqs - j, 1:2, :] = jnp.where(ok, jnp.exp(behind), 0.0)
        behind = behind + jnp.where(ok, tots[at, 1:2, :], 0.0)
        return ahead, behind

    zero = jnp.zeros((1, kw), F32)
    sums = (zero, zero)
    if seqs <= 16:
        for j in range(1, seqs):
            sums = weigh(j, sums)
    else:
        lax.fori_loop(1, seqs, weigh, sums)

    def gain(d, inflow):
        state_copy(d).wait_recv()
        part = recv[lax.rem(p - d + seqs, seqs)].astype(F32)
        return inflow[0] + part * wts[d, 0:1, :], inflow[1] + part * wts[d, 1:2, :]

    none = jnp.zeros((HEAD_V, kw), F32)
    inflow = (none, none)
    if seqs <= 16:
        for d in range(1, seqs):
            inflow = gain(d, inflow)
    else:
        inflow = lax.fori_loop(1, seqs, gain, inflow)
    spread = jnp.concatenate(
        [
            jnp.concatenate(
                [jnp.where(slane // HEAD_K == g, inflow[d], 0.0) for g in range(heads_here)], axis=0
            )
            for d in range(2)
        ],
        axis=1,
    ).astype(BF16)

    tail = HeadGather(heads, h, nrm.at[h], nrm, crows, ncs, ncr, nss, nsr)
    for c in range(CHUNKS):
        at = slice(c * crows, (c + 1) * crows)
        whole = mix[at, :] + lax.dot_general(qdev[at], spread, NT, preferred_element_type=F32)
        for g in range(heads_here):
            cols = slice(g * HEAD_V, (g + 1) * HEAD_V)
            part = whole[:, cols]
            scale = lax.rsqrt(jnp.mean(part * part, axis=-1, keepdims=True) + 1e-06)
            nrm[h, at, cols] = (part * scale * acc[at, cols]).astype(BF16)
        tail.start(c)

    for copy in wo_copies:
        copy.wait()
    for c in range(CHUNKS):
        at = slice(c * crows, (c + 1) * crows)
        total = dot(nrm[h, at, :], wo_s[h])
        tail.side(0, c).wait_recv()
        total += dot(nrm[tail.sib, at, :], wo_s[tail.sib])
        for j in range(1, tail.chips):
            tail.hand_on(j, c)
            origin = tail.cross_origin(j)
            total += dot(nrm[origin, at, :], wo_s[origin])
            tail.side(j, c).wait_recv()
            origin = tail.handed_origin(j)
            total += dot(nrm[origin, at, :], wo_s[origin])
        out_ref[at, :] = total.astype(BF16)

    gather.finish()
    tail.finish()
    each(seqs, 1, lambda d: total_copy(d).wait_send())
    each(seqs, 1, lambda d: state_copy(d).wait_send())


def solution(mesh):
    heads, seqs = mesh.shape["head"], mesh.shape["seq"]

    def local(features, w_query, w_key, w_value, w_gate, w_out, forget):
        rows, width = features.shape
        kw, vw = w_query.shape[1], w_value.shape[1]
        ow = w_out.shape[1] // heads
        blocks = rows // GROUP
        chips = heads // 2
        dma = pltpu.SemaphoreType.DMA
        hop = dma((chips, CHUNKS))
        return pl.pallas_call(
            functools.partial(kernel, heads, seqs),
            out_shape=jax.ShapeDtypeStruct((rows, ow), BF16),
            in_specs=[pl.BlockSpec(memory_space=pltpu.HBM)] * 7,
            out_specs=pl.BlockSpec(memory_space=pltpu.VMEM),
            scratch_shapes=[
                pltpu.VMEM((heads, rows, width), BF16),
                pltpu.VMEM((heads, width, 2 * (kw + vw)), BF16),
                pltpu.VMEM((heads, vw, ow), BF16),
                pltpu.VMEM((2, rows, kw), BF16),
                pltpu.VMEM((rows, 2 * (kw + vw)), F32),
                pltpu.VMEM((2, blocks + 3, rows, kw), F32),
                pltpu.VMEM((8, kw), F32),
                pltpu.VMEM((seqs, 8, kw), F32),
                pltpu.VMEM((seqs, 8, kw), F32),
                pltpu.VMEM((2, HEAD_V, kw), BF16),
                pltpu.VMEM((seqs, HEAD_V, kw), BF16),
                pltpu.VMEM((rows, vw), BF16),
                pltpu.VMEM((rows, kw), BF16),
                pltpu.VMEM((kw // HEAD_K, rows, rows), BF16),
                pltpu.VMEM((rows, vw), F32),
                pltpu.VMEM((heads, rows, vw), BF16),
                dma,
                dma((heads, 4)),
                dma((heads,)),
                dma,
                hop, hop, hop, hop, hop, hop, hop, hop,
                dma((seqs,)), dma((seqs,)), dma((seqs,)), dma((seqs,)),
                pltpu.SemaphoreType.REGULAR((max(1, (seqs - 1).bit_length()),)),
            ],
            compiler_params=pltpu.CompilerParams(
                collective_id=0, has_side_effects=True, vmem_limit_bytes=60 * 1024 * 1024
            ),
        )(features, w_query, w_key, w_value, w_gate, w_out, forget)

    placed = (
        P("seq", "head"),
        P(None, "head"),
        P(None, "head"),
        P(None, "head"),
        P(None, "head"),
        P(),
        P(None, "seq", "head"),
    )
    return jax.shard_map(
        local, mesh=mesh, in_specs=placed, out_specs=P("seq", "head"), check_vma=False
    )
```

```python
import functools

import jax
import jax.numpy as jnp
from jax import lax
from jax.experimental import pallas as pl
from jax.experimental.pallas import tpu as pltpu
from jax.sharding import PartitionSpec as P

HEAD_K = 64
HEAD_V = 128
GROUP = 64
CHUNKS = 2
MESH = pl.DeviceIdType.MESH
F32 = jnp.float32
BF16 = jnp.bfloat16
NT = (((1,), (1,)), ((), ()))
TN = (((0,), (0,)), ((), ()))


def dot(a, b):
    return jnp.dot(a, b, preferred_element_type=F32)


def each(count, start, body):
    if count - start <= 16:
        for i in range(start, count):
            body(i)
    else:
        lax.fori_loop(start, count, lambda i, c: (body(i), c)[1], 0)


class HeadGather:
    def __init__(self, heads, me, own, slots, rows, cs, cr, ss, sr):
        self.chips = heads // 2
        self.core = lax.rem(me, 2)
        self.chip = lax.div(me, 2)
        self.me, self.own, self.slots, self.rows = me, own, slots, rows
        self.sib = me + 1 - 2 * self.core
        self.cs, self.cr, self.ss, self.sr = cs, cr, ss, sr
        self.started = []

    def cut(self, ref, c):
        return ref.at[pl.ds(c * self.rows, self.rows), :]

    def cross_origin(self, j):
        return lax.rem(self.chip - j + self.chips, self.chips) * 2 + self.core

    def handed_origin(self, j):
        return lax.rem(self.chip - j + self.chips, self.chips) * 2 + 1 - self.core

    def cross(self, j, c):
        target = lax.rem(self.chip + j, self.chips) * 2 + self.core
        return pltpu.make_async_remote_copy(
            src_ref=self.cut(self.own, c),
            dst_ref=self.cut(self.slots.at[self.me], c),
            send_sem=self.cs.at[j, c],
            recv_sem=self.cr.at[j, c],
            device_id={"head": target},
            device_id_type=MESH,
        )

    def side(self, j, c):
        origin = self.me if j == 0 else self.cross_origin(j)
        src = self.own if j == 0 else self.slots.at[origin]
        return pltpu.make_async_remote_copy(
            src_ref=self.cut(src, c),
            dst_ref=self.cut(self.slots.at[origin], c),
            send_sem=self.ss.at[j, c],
            recv_sem=self.sr.at[j, c],
            device_id={"head": self.sib},
            device_id_type=MESH,
        )

    def start(self, c):
        for j in range(1, self.chips):
            copy = self.cross(j, c)
            copy.start()
            self.started.append(copy)
        copy = self.side(0, c)
        copy.start()
        self.started.append(copy)

    def hand_on(self, j, c):
        self.cross(j, c).wait_recv()
        copy = self.side(j, c)
        copy.start()
        self.started.append(copy)

    def finish(self):
        for copy in self.started:
            copy.wait_send()


def kernel(
    heads, seqs,
    feat_hbm, wq_hbm, wk_hbm, wv_hbm, wg_hbm, wo_hbm, forget_hbm,
    out_ref,
    feat, w_s, wo_s, fg, acc, mults, edge, tots, wts, st, recv, vals, keys, ps, mix, nrm,
    own_sem, w_sem, wo_sem, fg_sem,
    fcs, fcr, fss, fsr, ncs, ncr, nss, nsr, ts, tr, xs, xr, meet,
):
    h = lax.axis_index("head")
    p = lax.axis_index("seq")
    rows, width = feat_hbm.shape
    kw = wq_hbm.shape[1]
    vw = wv_hbm.shape[1]
    blocks = rows // GROUP
    crows = rows // CHUNKS
    k0, v0, q0, g0 = 0, kw, kw + vw, kw + vw + kw

    fg_copy = pltpu.make_async_copy(forget_hbm, fg, fg_sem)
    fg_copy.start()
    own_copy = pltpu.make_async_copy(feat_hbm, feat.at[h], own_sem)
    own_copy.start()
    w_copies = []
    for i in range(heads):
        for n, (src, at, wide) in enumerate(
            ((wk_hbm, k0, kw), (wv_hbm, v0, vw), (wq_hbm, q0, kw), (wg_hbm, g0, vw))
        ):
            copy = pltpu.make_async_copy(
                src.at[pl.ds(i * width, width), :],
                w_s.at[i, :, pl.ds(at, wide)],
                w_sem.at[i, n],
            )
            copy.start()
            w_copies.append(copy)
    wo_copies = []
    ow = out_ref.shape[1]
    for i in range(heads):
        copy = pltpu.make_async_copy(
            wo_hbm.at[pl.ds(i * vw, vw), pl.ds(pl.multiple_of(h * ow, ow), ow)],
            wo_s.at[i],
            wo_sem.at[i],
        )
        copy.start()
        wo_copies.append(copy)

    def near(sem, d):
        pl.semaphore_signal(
            sem, inc=1, device_id={"seq": p + 1 - 2 * lax.rem(p, 2)}, device_id_type=MESH
        )

        @pl.when(p >= d)
        def _():
            pl.semaphore_signal(sem, inc=1, device_id={"seq": p - d}, device_id_type=MESH)

        @pl.when(p + d < seqs)
        def _():
            pl.semaphore_signal(sem, inc=1, device_id={"seq": p + d}, device_id_type=MESH)

    def near_count(d):
        return 1 + jnp.where(p >= d, 1, 0) + jnp.where(p + d < seqs, 1, 0)

    barrier = pltpu.get_barrier_semaphore()
    sibling = h + 1 - 2 * lax.rem(h, 2)
    pl.semaphore_signal(barrier, inc=1, device_id={"head": sibling}, device_id_type=MESH)
    for j in range(2, heads, 2):
        pl.semaphore_signal(
            barrier, inc=1, device_id={"head": lax.rem(h + j, heads)}, device_id_type=MESH
        )
    near(barrier, 2)
    pl.semaphore_wait(barrier, heads // 2 + near_count(2))

    rounds = meet.shape[0]
    near(meet.at[0], 2)

    def met(r):
        pl.semaphore_wait(meet.at[r], near_count(2 << r))
        if r + 1 < rounds:
            near(meet.at[r + 1], 2 << (r + 1))

    gather = HeadGather(heads, h, feat_hbm, feat, crows, fcs, fcr, fss, fsr)
    for c in range(CHUNKS):
        gather.start(c)

    fg_copy.wait()
    tok = lax.broadcasted_iota(jnp.int32, (rows, rows), 0)
    src = lax.broadcasted_iota(jnp.int32, (rows, rows), 1)
    same = (tok // GROUP) == (src // GROUP)
    row = lax.broadcasted_iota(jnp.int32, (rows, kw), 0)
    lane = lax.broadcasted_iota(jnp.int32, (rows, kw), 1)
    edge[...] = jnp.zeros_like(edge)
    whole_sums, block_sums = [], []
    for d in range(2):
        order = (src <= tok) if d == 0 else (src >= tok)
        f = fg[d]
        whole = dot(jnp.where(order, 1.0, 0.0).astype(BF16), f)
        block = dot(jnp.where(order & same, 1.0, 0.0).astype(BF16), f)
        total = whole[rows - 1 : rows] if d == 0 else whole[0:1]
        edge[d : d + 1, :] = total
        whole_sums.append(whole)
        block_sums.append(block)

    met(0)

    def total_copy(d):
        return pltpu.make_async_remote_copy(
            src_ref=edge,
            dst_ref=tots.at[p],
            send_sem=ts.at[d],
            recv_sem=tr.at[d],
            device_id={"seq": lax.rem(p + d, seqs)},
            device_id_type=MESH,
        )

    for d in range(2):
        whole, block = whole_sums[d], block_sums[d]
        total = whole[rows - 1 : rows] if d == 0 else whole[0:1]
        mults[d, blocks] = jnp.exp(block)
        mults[d, blocks + 1] = jnp.exp(total - whole)
        mults[d, blocks + 2] = jnp.exp(whole)
        for i in range(blocks):
            lo, hi = i * GROUP, (i + 1) * GROUP
            inside = (row >= lo) & (row < hi)
            if d == 0:
                past = row < lo
                start = whole[lo - 1 : lo] if i else jnp.zeros((1, kw), F32)
            else:
                past = row >= hi
                start = whole[hi : hi + 1] if i < blocks - 1 else jnp.zeros((1, kw), F32)
            power = jnp.where(past, start - whole, jnp.where(inside, -block, -jnp.inf))
            mults[d, i] = jnp.exp(power)
    if rounds > 1:
        met(1)

    own_copy.wait()
    for copy in w_copies:
        copy.wait()
    acc[...] = dot(feat[h], w_s[h])
    gather.hand_on(1, 0)
    for r in range(2, rounds):
        met(r)
    each(seqs, 1, lambda d: total_copy(d).start())
    for c in range(CHUNKS):
        gather.side(0, c).wait_recv()
    acc[...] += dot(feat[gather.sib], w_s[gather.sib])
    for j in range(1, gather.chips):
        for c in range(CHUNKS):
            if j > 1 or c > 0:
                gather.hand_on(j, c)
        at = gather.cross_origin(j)
        if j < gather.chips - 1:
            acc[...] += dot(feat[at], w_s[at])
        else:
            acc[...] += dot(feat[at], w_s[at])
        for c in range(CHUNKS):
            gather.side(j, c).wait_recv()
        at = gather.handed_origin(j)
        if j < gather.chips - 1:
            acc[...] += dot(feat[at], w_s[at])
    last = gather.handed_origin(gather.chips - 1)
    kv = acc[:, :q0] + dot(feat[last], w_s[last, :, :q0])
    key = kv[:, :kw].astype(BF16)
    val = kv[:, kw:].astype(BF16)
    keys[...] = key
    vals[...] = val

    keyf = key.astype(F32)
    grown = jnp.concatenate(
        [(keyf * mults[d, blocks + 1]).astype(BF16) for d in range(2)], axis=1
    )
    state = lax.dot_general(val, grown, TN, preferred_element_type=F32)
    slane = lax.broadcasted_iota(jnp.int32, (HEAD_V, kw), 1)
    heads_here = kw // HEAD_K
    for d in range(2):
        packed = state[:HEAD_V, d * kw : (d + 1) * kw]
        for g in range(1, heads_here):
            packed = jnp.where(
                slane >= g * HEAD_K,
                state[g * HEAD_V : (g + 1) * HEAD_V, d * kw : (d + 1) * kw],
                packed,
            )
        st[d] = packed.astype(BF16)

    def state_copy(d):
        q = lax.rem(p + d, seqs)
        return pltpu.make_async_remote_copy(
            src_ref=st.at[jnp.where(q > p, 0, 1)],
            dst_ref=recv.at[p],
            send_sem=xs.at[d],
            recv_sem=xr.at[d],
            device_id={"seq": q},
            device_id_type=MESH,
        )

    each(seqs, 1, lambda d: state_copy(d).start())

    qg = acc[:, q0:] + dot(feat[last], w_s[last, :, q0:])
    query = (qg[:, :kw] * 0.125).astype(BF16).astype(F32)
    gate = qg[:, kw:]
    acc[:, :vw] = gate / (1.0 + jnp.exp(-gate))
    qd = [(query * mults[d, blocks]).astype(BF16) for d in range(2)]
    qdev = jnp.concatenate(
        [(query * mults[d, blocks + 2]).astype(BF16) for d in range(2)], axis=1
    )
    blane = lax.broadcasted_iota(jnp.int32, (GROUP, kw), 1) // HEAD_K
    bt = lax.rem(lax.broadcasted_iota(jnp.int32, (heads_here * GROUP, rows), 0), GROUP)
    bs = lax.broadcasted_iota(jnp.int32, (heads_here * GROUP, rows), 1)
    for i in range(blocks):
        scores = []
        for d in range(2):
            qb = qd[d][i * GROUP : (i + 1) * GROUP]
            stacked = jnp.concatenate(
                [jnp.where(blane == g, qb, jnp.zeros_like(qb)) for g in range(heads_here)], axis=0
            )
            grown_keys = (keyf * mults[d, i]).astype(BF16)
            part = lax.dot_general(stacked, grown_keys, NT, preferred_element_type=F32)
            keep = (bs <= bt + i * GROUP) if d == 0 else (bs >= bt + i * GROUP)
            scores.append(jnp.where(keep, part, 0.0))
        both = (scores[0] + scores[1]).astype(BF16)
        for g in range(heads_here):
            ps[g, i * GROUP : (i + 1) * GROUP, :] = both[g * GROUP : (g + 1) * GROUP]
    for g in range(heads_here):
        cols = slice(g * HEAD_V, (g + 1) * HEAD_V)
        mix[:, cols] = dot(ps[g], val[:, cols])

    each(seqs, 1, lambda d: total_copy(d).wait_recv())
    tots[p] = jnp.zeros_like(edge)

    def weigh(j, sums):
        ahead, behind = sums
        k = p - j
        ok = k >= 0
        at = jnp.maximum(k, 0)
        wts[j, 0:1, :] = jnp.where(ok, jnp.exp(ahead), 0.0)
        ahead = ahead + jnp.where(ok, tots[at, 0:1, :], 0.0)
        k = p + j
        ok = k < seqs
        at = jnp.minimum(k, seqs - 1)
        wts[seqs - j, 1:2, :] = jnp.where(ok, jnp.exp(behind), 0.0)
        behind = behind + jnp.where(ok, tots[at, 1:2, :], 0.0)
        return ahead, behind

    zero = jnp.zeros((1, kw), F32)
    sums = (zero, zero)
    if seqs <= 16:
        for j in range(1, seqs):
            sums = weigh(j, sums)
    else:
        lax.fori_loop(1, seqs, weigh, sums)

    def gain(d, inflow):
        state_copy(d).wait_recv()
        part = recv[lax.rem(p - d + seqs, seqs)].astype(F32)
        return inflow[0] + part * wts[d, 0:1, :], inflow[1] + part * wts[d, 1:2, :]

    none = jnp.zeros((HEAD_V, kw), F32)
    inflow = (none, none)
    if seqs <= 16:
        for d in range(1, seqs):
            inflow = gain(d, inflow)
    else:
        inflow = lax.fori_loop(1, seqs, gain, inflow)
    spread = jnp.concatenate(
        [
            jnp.concatenate(
                [jnp.where(slane // HEAD_K == g, inflow[d], 0.0) for g in range(heads_here)], axis=0
            )
            for d in range(2)
        ],
        axis=1,
    ).astype(BF16)

    tail = HeadGather(heads, h, nrm.at[h], nrm, crows, ncs, ncr, nss, nsr)
    for c in range(CHUNKS):
        at = slice(c * crows, (c + 1) * crows)
        whole = mix[at, :] + lax.dot_general(qdev[at], spread, NT, preferred_element_type=F32)
        for g in range(heads_here):
            cols = slice(g * HEAD_V, (g + 1) * HEAD_V)
            part = whole[:, cols]
            scale = lax.rsqrt(jnp.mean(part * part, axis=-1, keepdims=True) + 1e-06)
            nrm[h, at, cols] = (part * scale * acc[at, cols]).astype(BF16)
        tail.start(c)

    for copy in wo_copies:
        copy.wait()
    for c in range(CHUNKS):
        at = slice(c * crows, (c + 1) * crows)
        total = dot(nrm[h, at, :], wo_s[h])
        tail.side(0, c).wait_recv()
        total += dot(nrm[tail.sib, at, :], wo_s[tail.sib])
        for j in range(1, tail.chips):
            tail.hand_on(j, c)
            origin = tail.cross_origin(j)
            total += dot(nrm[origin, at, :], wo_s[origin])
            tail.side(j, c).wait_recv()
            origin = tail.handed_origin(j)
            total += dot(nrm[origin, at, :], wo_s[origin])
        out_ref[at, :] = total.astype(BF16)

    gather.finish()
    tail.finish()
    each(seqs, 1, lambda d: total_copy(d).wait_send())
    each(seqs, 1, lambda d: state_copy(d).wait_send())


def solution(mesh):
    heads, seqs = mesh.shape["head"], mesh.shape["seq"]

    def local(features, w_query, w_key, w_value, w_gate, w_out, forget):
        rows, width = features.shape
        kw, vw = w_query.shape[1], w_value.shape[1]
        ow = w_out.shape[1] // heads
        blocks = rows // GROUP
        chips = heads // 2
        dma = pltpu.SemaphoreType.DMA
        hop = dma((chips, CHUNKS))
        return pl.pallas_call(
            functools.partial(kernel, heads, seqs),
            out_shape=jax.ShapeDtypeStruct((rows, ow), BF16),
            in_specs=[pl.BlockSpec(memory_space=pltpu.HBM)] * 7,
            out_specs=pl.BlockSpec(memory_space=pltpu.VMEM),
            scratch_shapes=[
                pltpu.VMEM((heads, rows, width), BF16),
                pltpu.VMEM((heads, width, 2 * (kw + vw)), BF16),
                pltpu.VMEM((heads, vw, ow), BF16),
                pltpu.VMEM((2, rows, kw), BF16),
                pltpu.VMEM((rows, 2 * (kw + vw)), F32),
                pltpu.VMEM((2, blocks + 3, rows, kw), F32),
                pltpu.VMEM((8, kw), F32),
                pltpu.VMEM((seqs, 8, kw), F32),
                pltpu.VMEM((seqs, 8, kw), F32),
                pltpu.VMEM((2, HEAD_V, kw), BF16),
                pltpu.VMEM((seqs, HEAD_V, kw), BF16),
                pltpu.VMEM((rows, vw), BF16),
                pltpu.VMEM((rows, kw), BF16),
                pltpu.VMEM((kw // HEAD_K, rows, rows), BF16),
                pltpu.VMEM((rows, vw), F32),
                pltpu.VMEM((heads, rows, vw), BF16),
                dma,
                dma((heads, 4)),
                dma((heads,)),
                dma,
                hop, hop, hop, hop, hop, hop, hop, hop,
                dma((seqs,)), dma((seqs,)), dma((seqs,)), dma((seqs,)),
                pltpu.SemaphoreType.REGULAR((max(1, (seqs // 2 - 1).bit_length()),)),
            ],
            compiler_params=pltpu.CompilerParams(
                collective_id=0, has_side_effects=True, vmem_limit_bytes=56400000
            ),
        )(features, w_query, w_key, w_value, w_gate, w_out, forget)

    placed = (
        P("seq", "head"),
        P(None, "head"),
        P(None, "head"),
        P(None, "head"),
        P(None, "head"),
        P(),
        P(None, "seq", "head"),
    )
    return jax.shard_map(
        local, mesh=mesh, in_specs=placed, out_specs=P("seq", "head"), check_vma=False
    )
```

```python
import functools

import jax
import jax.numpy as jnp
from jax import lax
from jax.experimental import pallas as pl
from jax.experimental.pallas import tpu as pltpu
from jax.sharding import PartitionSpec as P

HEAD_K = 64
HEAD_V = 128
GROUP = 64
CHUNKS = 2
MESH = pl.DeviceIdType.MESH
F32 = jnp.float32
BF16 = jnp.bfloat16
NT = (((1,), (1,)), ((), ()))
TN = (((0,), (0,)), ((), ()))


def dot(a, b):
    return jnp.dot(a, b, preferred_element_type=F32)


def each(count, start, body):
    if count - start <= 16:
        for i in range(start, count):
            body(i)
    else:
        lax.fori_loop(start, count, lambda i, c: (body(i), c)[1], 0)


class HeadGather:
    def __init__(self, heads, me, own, slots, rows, cs, cr, ss, sr):
        self.chips = heads // 2
        self.core = lax.rem(me, 2)
        self.chip = lax.div(me, 2)
        self.me, self.own, self.slots, self.rows = me, own, slots, rows
        self.sib = me + 1 - 2 * self.core
        self.cs, self.cr, self.ss, self.sr = cs, cr, ss, sr
        self.started = []

    def cut(self, ref, c):
        return ref.at[pl.ds(c * self.rows, self.rows), :]

    def cross_origin(self, j):
        return lax.rem(self.chip - j + self.chips, self.chips) * 2 + self.core

    def handed_origin(self, j):
        return lax.rem(self.chip - j + self.chips, self.chips) * 2 + 1 - self.core

    def cross(self, j, c):
        target = lax.rem(self.chip + j, self.chips) * 2 + self.core
        return pltpu.make_async_remote_copy(
            src_ref=self.cut(self.own, c),
            dst_ref=self.cut(self.slots.at[self.me], c),
            send_sem=self.cs.at[j, c],
            recv_sem=self.cr.at[j, c],
            device_id={"head": target},
            device_id_type=MESH,
        )

    def side(self, j, c):
        origin = self.me if j == 0 else self.cross_origin(j)
        src = self.own if j == 0 else self.slots.at[origin]
        return pltpu.make_async_remote_copy(
            src_ref=self.cut(src, c),
            dst_ref=self.cut(self.slots.at[origin], c),
            send_sem=self.ss.at[j, c],
            recv_sem=self.sr.at[j, c],
            device_id={"head": self.sib},
            device_id_type=MESH,
        )

    def start(self, c):
        for j in range(1, self.chips):
            copy = self.cross(j, c)
            copy.start()
            self.started.append(copy)
        copy = self.side(0, c)
        copy.start()
        self.started.append(copy)

    def hand_on(self, j, c):
        self.cross(j, c).wait_recv()
        copy = self.side(j, c)
        copy.start()
        self.started.append(copy)

    def finish(self):
        for copy in self.started:
            copy.wait_send()


def kernel(
    heads, seqs,
    feat_hbm, wq_hbm, wk_hbm, wv_hbm, wg_hbm, wo_hbm, forget_hbm,
    out_ref,
    feat, w_s, wo_s, fg, acc, mults, edge, tots, wts, st, recv, vals, keys, ps, mix, nrm,
    own_sem, w_sem, wo_sem, fg_sem,
    fcs, fcr, fss, fsr, ncs, ncr, nss, nsr, ts, tr, xs, xr, meet,
):
    h = lax.axis_index("head")
    p = lax.axis_index("seq")
    rows, width = feat_hbm.shape
    kw = wq_hbm.shape[1]
    vw = wv_hbm.shape[1]
    blocks = rows // GROUP
    crows = rows // CHUNKS
    k0, v0, q0, g0 = 0, kw, kw + vw, kw + vw + kw

    fg_copy = pltpu.make_async_copy(forget_hbm, fg, fg_sem)
    fg_copy.start()
    own_copy = pltpu.make_async_copy(feat_hbm, feat.at[h], own_sem)
    own_copy.start()
    w_copies = []
    for i in range(heads):
        for n, (src, at, wide) in enumerate(
            ((wk_hbm, k0, kw), (wv_hbm, v0, vw), (wq_hbm, q0, kw), (wg_hbm, g0, vw))
        ):
            copy = pltpu.make_async_copy(
                src.at[pl.ds(i * width, width), :],
                w_s.at[i, :, pl.ds(at, wide)],
                w_sem.at[i, n],
            )
            copy.start()
            w_copies.append(copy)
    wo_copies = []
    ow = out_ref.shape[1]
    for i in range(heads):
        copy = pltpu.make_async_copy(
            wo_hbm.at[pl.ds(i * vw, vw), pl.ds(pl.multiple_of(h * ow, ow), ow)],
            wo_s.at[i],
            wo_sem.at[i],
        )
        copy.start()
        wo_copies.append(copy)

    def near(sem, d):
        pl.semaphore_signal(
            sem, inc=1, device_id={"seq": p + 1 - 2 * lax.rem(p, 2)}, device_id_type=MESH
        )

        @pl.when(p >= d)
        def _():
            pl.semaphore_signal(sem, inc=1, device_id={"seq": p - d}, device_id_type=MESH)

        @pl.when(p + d < seqs)
        def _():
            pl.semaphore_signal(sem, inc=1, device_id={"seq": p + d}, device_id_type=MESH)

    def near_count(d):
        return 1 + jnp.where(p >= d, 1, 0) + jnp.where(p + d < seqs, 1, 0)

    barrier = pltpu.get_barrier_semaphore()
    sibling = h + 1 - 2 * lax.rem(h, 2)
    pl.semaphore_signal(barrier, inc=1, device_id={"head": sibling}, device_id_type=MESH)
    for j in range(2, heads, 2):
        pl.semaphore_signal(
            barrier, inc=1, device_id={"head": lax.rem(h + j, heads)}, device_id_type=MESH
        )
    near(barrier, 2)
    pl.semaphore_wait(barrier, heads // 2 + near_count(2))

    rounds = meet.shape[0]
    near(meet.at[0], 2)

    def met(r):
        pl.semaphore_wait(meet.at[r], near_count(2 << r))
        if r + 1 < rounds:
            near(meet.at[r + 1], 2 << (r + 1))

    own_copy.wait()
    gather = HeadGather(heads, h, feat.at[h], feat, crows, fcs, fcr, fss, fsr)
    for c in range(CHUNKS):
        gather.start(c)

    fg_copy.wait()
    tok = lax.broadcasted_iota(jnp.int32, (rows, rows), 0)
    src = lax.broadcasted_iota(jnp.int32, (rows, rows), 1)
    same = (tok // GROUP) == (src // GROUP)
    row = lax.broadcasted_iota(jnp.int32, (rows, kw), 0)
    lane = lax.broadcasted_iota(jnp.int32, (rows, kw), 1)
    edge[...] = jnp.zeros_like(edge)
    whole_sums, block_sums = [], []
    for d in range(2):
        order = (src <= tok) if d == 0 else (src >= tok)
        f = fg[d]
        whole = dot(jnp.where(order, 1.0, 0.0).astype(BF16), f)
        block = dot(jnp.where(order & same, 1.0, 0.0).astype(BF16), f)
        total = whole[rows - 1 : rows] if d == 0 else whole[0:1]
        edge[d : d + 1, :] = total
        whole_sums.append(whole)
        block_sums.append(block)

    met(0)

    def total_copy(d):
        return pltpu.make_async_remote_copy(
            src_ref=edge,
            dst_ref=tots.at[p],
            send_sem=ts.at[d],
            recv_sem=tr.at[d],
            device_id={"seq": lax.rem(p + d, seqs)},
            device_id_type=MESH,
        )

    for d in range(2):
        whole, block = whole_sums[d], block_sums[d]
        total = whole[rows - 1 : rows] if d == 0 else whole[0:1]
        mults[d, blocks] = jnp.exp(block)
        mults[d, blocks + 1] = jnp.exp(total - whole)
        mults[d, blocks + 2] = jnp.exp(whole)
        for i in range(blocks):
            lo, hi = i * GROUP, (i + 1) * GROUP
            inside = (row >= lo) & (row < hi)
            if d == 0:
                past = row < lo
                start = whole[lo - 1 : lo] if i else jnp.zeros((1, kw), F32)
            else:
                past = row >= hi
                start = whole[hi : hi + 1] if i < blocks - 1 else jnp.zeros((1, kw), F32)
            power = jnp.where(past, start - whole, jnp.where(inside, -block, -jnp.inf))
            mults[d, i] = jnp.exp(power)
    if rounds > 1:
        met(1)

    for copy in w_copies:
        copy.wait()
    acc[...] = dot(feat[h], w_s[h])
    gather.hand_on(1, 0)
    for r in range(2, rounds):
        met(r)
    each(seqs, 1, lambda d: total_copy(d).start())
    for c in range(CHUNKS):
        gather.side(0, c).wait_recv()
    acc[...] += dot(feat[gather.sib], w_s[gather.sib])
    for j in range(1, gather.chips):
        for c in range(CHUNKS):
            if j > 1 or c > 0:
                gather.hand_on(j, c)
        at = gather.cross_origin(j)
        if j < gather.chips - 1:
            acc[...] += dot(feat[at], w_s[at])
        else:
            acc[...] += dot(feat[at], w_s[at])
        for c in range(CHUNKS):
            gather.side(j, c).wait_recv()
        at = gather.handed_origin(j)
        if j < gather.chips - 1:
            acc[...] += dot(feat[at], w_s[at])
    last = gather.handed_origin(gather.chips - 1)
    kv = acc[:, :q0] + dot(feat[last], w_s[last, :, :q0])
    key = kv[:, :kw].astype(BF16)
    val = kv[:, kw:].astype(BF16)
    keys[...] = key
    vals[...] = val

    keyf = key.astype(F32)
    grown = jnp.concatenate(
        [(keyf * mults[d, blocks + 1]).astype(BF16) for d in range(2)], axis=1
    )
    state = lax.dot_general(val, grown, TN, preferred_element_type=F32)
    slane = lax.broadcasted_iota(jnp.int32, (HEAD_V, kw), 1)
    heads_here = kw // HEAD_K
    for d in range(2):
        packed = state[:HEAD_V, d * kw : (d + 1) * kw]
        for g in range(1, heads_here):
            packed = jnp.where(
                slane >= g * HEAD_K,
                state[g * HEAD_V : (g + 1) * HEAD_V, d * kw : (d + 1) * kw],
                packed,
            )
        st[d] = packed.astype(BF16)

    def state_copy(d):
        q = lax.rem(p + d, seqs)
        return pltpu.make_async_remote_copy(
            src_ref=st.at[jnp.where(q > p, 0, 1)],
            dst_ref=recv.at[p],
            send_sem=xs.at[d],
            recv_sem=xr.at[d],
            device_id={"seq": q},
            device_id_type=MESH,
        )

    each(seqs, 1, lambda d: state_copy(d).start())

    qg = acc[:, q0:] + dot(feat[last], w_s[last, :, q0:])
    query = (qg[:, :kw] * 0.125).astype(BF16).astype(F32)
    gate = qg[:, kw:]
    acc[:, :vw] = gate / (1.0 + jnp.exp(-gate))
    qd = [(query * mults[d, blocks]).astype(BF16) for d in range(2)]
    qdev = jnp.concatenate(
        [(query * mults[d, blocks + 2]).astype(BF16) for d in range(2)], axis=1
    )
    blane = lax.broadcasted_iota(jnp.int32, (GROUP, kw), 1) // HEAD_K
    bt = lax.rem(lax.broadcasted_iota(jnp.int32, (heads_here * GROUP, rows), 0), GROUP)
    bs = lax.broadcasted_iota(jnp.int32, (heads_here * GROUP, rows), 1)
    for i in range(blocks):
        scores = []
        for d in range(2):
            qb = qd[d][i * GROUP : (i + 1) * GROUP]
            stacked = jnp.concatenate(
                [jnp.where(blane == g, qb, jnp.zeros_like(qb)) for g in range(heads_here)], axis=0
            )
            grown_keys = (keyf * mults[d, i]).astype(BF16)
            part = lax.dot_general(stacked, grown_keys, NT, preferred_element_type=F32)
            keep = (bs <= bt + i * GROUP) if d == 0 else (bs >= bt + i * GROUP)
            scores.append(jnp.where(keep, part, 0.0))
        both = (scores[0] + scores[1]).astype(BF16)
        for g in range(heads_here):
            ps[g, i * GROUP : (i + 1) * GROUP, :] = both[g * GROUP : (g + 1) * GROUP]
    for g in range(heads_here):
        cols = slice(g * HEAD_V, (g + 1) * HEAD_V)
        mix[:, cols] = dot(ps[g], val[:, cols])

    each(seqs, 1, lambda d: total_copy(d).wait_recv())
    tots[p] = jnp.zeros_like(edge)

    def weigh(j, sums):
        ahead, behind = sums
        k = p - j
        ok = k >= 0
        at = jnp.maximum(k, 0)
        wts[j, 0:1, :] = jnp.where(ok, jnp.exp(ahead), 0.0)
        ahead = ahead + jnp.where(ok, tots[at, 0:1, :], 0.0)
        k = p + j
        ok = k < seqs
        at = jnp.minimum(k, seqs - 1)
        wts[seqs - j, 1:2, :] = jnp.where(ok, jnp.exp(behind), 0.0)
        behind = behind + jnp.where(ok, tots[at, 1:2, :], 0.0)
        return ahead, behind

    zero = jnp.zeros((1, kw), F32)
    sums = (zero, zero)
    if seqs <= 16:
        for j in range(1, seqs):
            sums = weigh(j, sums)
    else:
        lax.fori_loop(1, seqs, weigh, sums)

    def gain(d, inflow):
        state_copy(d).wait_recv()
        part = recv[lax.rem(p - d + seqs, seqs)].astype(F32)
        return inflow[0] + part * wts[d, 0:1, :], inflow[1] + part * wts[d, 1:2, :]

    none = jnp.zeros((HEAD_V, kw), F32)
    inflow = (none, none)
    if seqs <= 16:
        for d in range(1, seqs):
            inflow = gain(d, inflow)
    else:
        inflow = lax.fori_loop(1, seqs, gain, inflow)
    spread = jnp.concatenate(
        [
            jnp.concatenate(
                [jnp.where(slane // HEAD_K == g, inflow[d], 0.0) for g in range(heads_here)], axis=0
            )
            for d in range(2)
        ],
        axis=1,
    ).astype(BF16)

    tail = HeadGather(heads, h, nrm.at[h], nrm, crows, ncs, ncr, nss, nsr)
    for c in range(CHUNKS):
        at = slice(c * crows, (c + 1) * crows)
        whole = mix[at, :] + lax.dot_general(qdev[at], spread, NT, preferred_element_type=F32)
        for g in range(heads_here):
            cols = slice(g * HEAD_V, (g + 1) * HEAD_V)
            part = whole[:, cols]
            scale = lax.rsqrt(jnp.mean(part * part, axis=-1, keepdims=True) + 1e-06)
            nrm[h, at, cols] = (part * scale * acc[at, cols]).astype(BF16)
        tail.start(c)

    for copy in wo_copies:
        copy.wait()
    for c in range(CHUNKS):
        at = slice(c * crows, (c + 1) * crows)
        total = dot(nrm[h, at, :], wo_s[h])
        tail.side(0, c).wait_recv()
        total += dot(nrm[tail.sib, at, :], wo_s[tail.sib])
        for j in range(1, tail.chips):
            tail.hand_on(j, c)
            origin = tail.cross_origin(j)
            total += dot(nrm[origin, at, :], wo_s[origin])
            tail.side(j, c).wait_recv()
            origin = tail.handed_origin(j)
            total += dot(nrm[origin, at, :], wo_s[origin])
        out_ref[at, :] = total.astype(BF16)

    gather.finish()
    tail.finish()
    each(seqs, 1, lambda d: total_copy(d).wait_send())
    each(seqs, 1, lambda d: state_copy(d).wait_send())


def solution(mesh):
    heads, seqs = mesh.shape["head"], mesh.shape["seq"]

    def local(features, w_query, w_key, w_value, w_gate, w_out, forget):
        rows, width = features.shape
        kw, vw = w_query.shape[1], w_value.shape[1]
        ow = w_out.shape[1] // heads
        blocks = rows // GROUP
        chips = heads // 2
        dma = pltpu.SemaphoreType.DMA
        hop = dma((chips, CHUNKS))
        return pl.pallas_call(
            functools.partial(kernel, heads, seqs),
            out_shape=jax.ShapeDtypeStruct((rows, ow), BF16),
            in_specs=[pl.BlockSpec(memory_space=pltpu.HBM)] * 7,
            out_specs=pl.BlockSpec(memory_space=pltpu.VMEM),
            scratch_shapes=[
                pltpu.VMEM((heads, rows, width), BF16),
                pltpu.VMEM((heads, width, 2 * (kw + vw)), BF16),
                pltpu.VMEM((heads, vw, ow), BF16),
                pltpu.VMEM((2, rows, kw), BF16),
                pltpu.VMEM((rows, 2 * (kw + vw)), F32),
                pltpu.VMEM((2, blocks + 3, rows, kw), F32),
                pltpu.VMEM((8, kw), F32),
                pltpu.VMEM((seqs, 8, kw), F32),
                pltpu.VMEM((seqs, 8, kw), F32),
                pltpu.VMEM((2, HEAD_V, kw), BF16),
                pltpu.VMEM((seqs, HEAD_V, kw), BF16),
                pltpu.VMEM((rows, vw), BF16),
                pltpu.VMEM((rows, kw), BF16),
                pltpu.VMEM((kw // HEAD_K, rows, rows), BF16),
                pltpu.VMEM((rows, vw), F32),
                pltpu.VMEM((heads, rows, vw), BF16),
                dma,
                dma((heads, 4)),
                dma((heads,)),
                dma,
                hop, hop, hop, hop, hop, hop, hop, hop,
                dma((seqs,)), dma((seqs,)), dma((seqs,)), dma((seqs,)),
                pltpu.SemaphoreType.REGULAR((max(1, (seqs // 2 - 1).bit_length()),)),
            ],
            compiler_params=pltpu.CompilerParams(
                collective_id=0, has_side_effects=True, vmem_limit_bytes=56400000
            ),
        )(features, w_query, w_key, w_value, w_gate, w_out, forget)

    placed = (
        P("seq", "head"),
        P(None, "head"),
        P(None, "head"),
        P(None, "head"),
        P(None, "head"),
        P(),
        P(None, "seq", "head"),
    )
    return jax.shard_map(
        local, mesh=mesh, in_specs=placed, out_specs=P("seq", "head"), check_vma=False
    )
```
